1024 devices in a mesh: gx: 256 (over y, z, core), gy: 4 (over x).
Axes of the slice: x: 4, y: 8, z: 16, core: 2. Of those that a mesh axis runs over, the one named last changes fastest.
Arguments:
- populations: float32 [19, 1024, 32, 128], P(None, 'gx', 'gy'), may hold values from 0.02 to 0.1
- fluid: int32 [1024, 32, 128], P('gx', 'gy'), may hold values 0 or 1
Outputs:
- advanced: float32 [19, 1024, 32, 128], P(None, 'gx', 'gy')
The draws below stay inside these ranges and needn't reach their ends.
Inputs may be any that keep to these rules, and one draw needn't show every extreme that they name: 1 marks a fluid cell, 0 a solid one.
All inputs are finite; a program needn't handle non-finite values. No bound on the sum of `fluid` on one device may be relied on, other than what follows from the above.
Results may differ from the reference program's by a relative error of at most 0.0001.
Values sent between devices are 32-bit elements; how exact they have to be, the bound alone decides.
A program may use at most 32 MiB of HBM per device.

```python
import jax
import jax.numpy as jnp
import numpy as np
from jax import lax

NZ = 128
STEPS = 4
NX = 1024
NY = 32


def with_ends(values, rng, least, high):
    place = [jax.random.randint(jax.random.fold_in(rng, axis), (), 0, length) for axis, length in enumerate(values.shape)]
    longest = values.shape.index(max(values.shape))
    beside = place[:longest] + [(place[longest] + 1) % values.shape[longest]] + place[longest + 1:]
    return values.at[tuple(place)].set(least).at[tuple(beside)].set(high)


def level_of(own_key, dims, pieces, low, largest):
    loudness = 1.0
    for axis_at, parts in pieces:
        steps = jax.random.uniform(jax.random.fold_in(jax.random.fold_in(own_key, 6), axis_at), (parts,), jnp.float32, low / len(pieces), largest / len(pieces))
        loudness = loudness * jnp.repeat(jnp.exp(steps), dims[axis_at] // parts).reshape((-1,) + (1,) * (len(dims) - 1 - axis_at))
    return loudness


def setup_inputs(seed: int = 0) -> dict:
    keys = jax.random.split(jax.random.key(seed), 3)
    populations = jnp.clip(0.02 + 0.08 * jax.random.uniform(keys[0], (19, NX, NY, NZ), jnp.float32) ** level_of(keys[0], (19, NX, NY, NZ), ((1, 256), (2, 4)), -0.2, 0.2), 0.02, 0.1)
    fluid = with_ends((jax.random.randint(keys[1], (NX, NY, NZ), 0, 8) < 7).astype(jnp.int32), jax.random.fold_in(keys[1], 1), 0, 1)
    return {"populations": populations, "fluid": fluid}


VELOCITIES = np.array([[0, 0, 0], [1, 0, 0], [-1, 0, 0], [0, 1, 0], [0, -1, 0], [0, 0, 1], [0, 0, -1], [1, 1, 0], [-1, -1, 0], [1, -1, 0], [-1, 1, 0], [1, 0, 1], [-1, 0, -1], [1, 0, -1], [-1, 0, 1], [0, 1, 1], [0, -1, -1], [0, 1, -1], [0, -1, 1]])
OPPOSITE = [0, 2, 1, 4, 3, 6, 5, 8, 7, 10, 9, 12, 11, 14, 13, 16, 15, 18, 17]
WEIGHTS = [1.0 / 3.0] + [1.0 / 18.0] * 6 + [1.0 / 36.0] * 12
relax_rate = 1.25


def lattice_step(pops, wet):
    vel = jnp.asarray(VELOCITIES.T.astype(np.float32))
    weights = jnp.asarray(np.array(WEIGHTS, np.float32))
    rho = jnp.sum(pops, axis=0)
    moment = jnp.einsum("dq,qabz->dabz", vel, pops, precision=lax.Precision.HIGHEST)
    speed = moment / rho[None]
    usq = jnp.sum(speed * speed, axis=0)
    proj = jnp.einsum("dq,dabz->qabz", vel, speed, precision=lax.Precision.HIGHEST)
    feq = weights[:, None, None, None] * rho[None] * (1.0 + 3.0 * proj + 4.5 * proj * proj - 1.5 * usq[None])
    post = jnp.where(wet[None], pops + relax_rate * (feq - pops), pops)
    sizea, sizeb = pops.shape[1], pops.shape[2]
    here = wet[1:-1, 1:-1]
    result = []
    for q in range(19):
        cx, cy, cz = int(VELOCITIES[q, 0]), int(VELOCITIES[q, 1]), int(VELOCITIES[q, 2])
        source = jnp.roll(post[q, 1 - cx:sizea - 1 - cx, 1 - cy:sizeb - 1 - cy], cz, axis=-1)
        source_wet = jnp.roll(wet[1 - cx:sizea - 1 - cx, 1 - cy:sizeb - 1 - cy], cz, axis=-1)
        bounced = post[OPPOSITE[q], 1:-1, 1:-1]
        result.append(jnp.where(here, jnp.where(source_wet, source, bounced), post[q, 1:-1, 1:-1]))
    return jnp.stack(result)


def reference(populations, fluid):
    wet = fluid == 1
    current = populations
    for step in range(STEPS):
        padded = jnp.pad(current, ((0, 0), (1, 1), (0, 0), (0, 0)), mode="wrap")
        padded = jnp.pad(padded, ((0, 0), (0, 0), (1, 1), (0, 0)))
        wet_pad = jnp.pad(wet, ((1, 1), (0, 0), (0, 0)), mode="wrap")
        wet_pad = jnp.pad(wet_pad, ((0, 0), (1, 1), (0, 0)))
        current = lattice_step(padded, wet_pad)
    return current
```

```python
import functools

import jax
import jax.numpy as jnp
from jax import lax
from jax.experimental import pallas as pl
from jax.experimental.pallas import tpu as pltpu
from jax.sharding import PartitionSpec as P

MESH = pl.DeviceIdType.MESH
F32 = jnp.float32

VEL = [
    (0, 0, 0), (1, 0, 0), (-1, 0, 0), (0, 1, 0), (0, -1, 0), (0, 0, 1), (0, 0, -1),
    (1, 1, 0), (-1, -1, 0), (1, -1, 0), (-1, 1, 0), (1, 0, 1), (-1, 0, -1), (1, 0, -1), (-1, 0, 1),
    (0, 1, 1), (0, -1, -1), (0, 1, -1), (0, -1, 1),
]
OPP = [0, 2, 1, 4, 3, 6, 5, 8, 7, 10, 9, 12, 11, 14, 13, 16, 15, 18, 17]
OMEGA = 1.25
ORDER = [2, 8, 10, 12, 14, 0, 3, 4, 5, 6, 15, 16, 17, 18, 1, 7, 9, 11, 13]
SLOT = [ORDER.index(q) for q in range(19)]
LEFT, RIGHT = 0, 1
BELOW, ABOVE = 0, 1


def relax(f):
    even = {q: f[q] + f[q + 1] for q in range(1, 19, 2)}
    odd = {q: f[q] - f[q + 1] for q in range(1, 19, 2)}
    rho = (((f[0] + even[1]) + (even[3] + even[5])) + ((even[7] + even[9]) + (even[11] + even[13]))) + (even[15] + even[17])
    jx = (odd[1] + odd[7]) + (odd[9] + odd[11]) + odd[13]
    jy = (odd[3] + odd[7]) + (odd[15] - odd[9]) + odd[17]
    jz = (odd[5] + odd[11]) + (odd[15] - odd[13]) - odd[17]
    inv = 3.0 / rho
    v = (jx * inv, jy * inv, jz * inv)
    base = 1.0 - (v[0] * v[0] + v[1] * v[1] + v[2] * v[2]) * (1.5 / 9.0)
    out = [None] * 19
    keep = 1.0 - OMEGA
    out[0] = f[0] * keep + (rho * (OMEGA / 3.0)) * base
    for first, last, weight in ((1, 7, 1.0 / 18.0), (7, 19, 1.0 / 36.0)):
        scale = rho * (OMEGA * weight)
        level = scale * base
        half = scale * 0.5
        for q in range(first, last, 2):
            proj = None
            for axis in range(3):
                c = VEL[q][axis]
                if c:
                    term = v[axis]
                    if proj is None:
                        proj = term
                    else:
                        proj = proj + term if c > 0 else proj - term
            sym = level + half * (proj * proj)
            anti = scale * proj
            out[q] = f[q] * keep + (sym + anti)
            out[q + 1] = f[q + 1] * keep + (sym - anti)
    return out


def pulled(grid, masks, level, col, start):
    f = []
    for q in range(19):
        cx, cy, cz = VEL[q]
        src = grid[level, col - cx, SLOT[q], pl.ds(start - cy, 8), :]
        if q == 0:
            f.append(src)
            continue
        if cz:
            src = pltpu.roll(src, cz % 128, 1)
        open_ = masks[col, q - 1, pl.ds(start, 8), :] > 0.5
        f.append(jnp.where(open_, src, grid[level, col, SLOT[OPP[q]], pl.ds(start, 8), :]))
    return f


def column_step(grid, masks, level, col):
    for start in (1, 7):
        post = relax(pulled(grid, masks, level, col, start))
        for q in range(19):
            grid[level + 1, col, SLOT[q], pl.ds(start, 8), :] = post[q]


def mask_column(marks, masks, col):
    for start in (1, 7):
        for q in range(1, 19):
            cx, cy, cz = VEL[q]
            wet = marks[col - cx, pl.ds(start - cy, 8), :]
            if cz:
                wet = pltpu.roll(wet, cz % 128, 1)
            masks[col, q - 1, pl.ds(start, 8), :] = wet


def kernel(nx, ny, zs, pop_ref, fluid_ref, out_ref, f0, wet_in, xs, ms, xr, mxr, yr, myr, cr, mcr, grid, marks, masks,
           load_sem, send_sem, recv_sem):
    gx, gy = lax.axis_index("gx"), lax.axis_index("gy")
    right, left = lax.rem(gx + 1, nx), lax.rem(gx + nx - 1, nx)
    has = (gy > 0, gy < ny - 1)
    seam = lax.rem(gx, zs) == 0

    load_fluid = pltpu.make_async_copy(fluid_ref, wet_in, load_sem.at[4])
    load_fluid.start()
    loads = [pltpu.make_async_copy(pop_ref.at[:, c], f0.at[:, c], load_sem.at[c]) for c in range(4)]
    for c in (3, 2, 1, 0):
        loads[c].start()

    barrier = pltpu.get_barrier_semaphore()
    pl.semaphore_signal(barrier, inc=1, device_id=(left, gy), device_id_type=MESH)
    for d, step in ((BELOW, -1), (ABOVE, 1)):
        @pl.when(has[d])
        def _():
            pl.semaphore_signal(barrier, inc=1, device_id=(gx, gy + step), device_id_type=MESH)

    def copy(number, src, dst, device):
        return pltpu.make_async_remote_copy(
            src_ref=src, dst_ref=dst, send_sem=send_sem.at[number], recv_sem=recv_sem.at[number],
            device_id=device, device_id_type=MESH)

    def to_x(side, k):
        device = (right, gy) if side == LEFT else (left, gy)
        number = side * 5 + k
        if k == 0:
            return copy(number, ms, mxr.at[side], device)
        c = 4 - k if side == LEFT else k - 1
        if k < 4:
            return copy(number, xs.at[c], xr.at[side, k - 1], device)
        part = pl.ds(14, 5) if side == LEFT else pl.ds(0, 5)
        return copy(number, xs.at[c, :, part], xr.at[side, k - 1, :, part], device)

    def to_y(d, k):
        device = (gx, gy + 1) if d == BELOW else (gx, gy - 1)
        h = 1 - d
        number = 10 + 2 * d + k
        if k == 0:
            return copy(number, ms.at[:, h], myr.at[d], device)
        return copy(number, xs.at[:, h], yr.at[d], device)

    def to_corner(d, side, k):
        device = (gx, gy + 1) if d == BELOW else (gx, gy - 1)
        h = 1 - d
        number = 14 + (d * 2 + side) * 5 + k
        if k == 0:
            return copy(number, mxr.at[side, :, h], mcr.at[d, side], device)
        if k < 4:
            return copy(number, xr.at[side, k - 1, h], cr.at[d, side, k - 1], device)
        part = pl.ds(14, 5) if side == LEFT else pl.ds(0, 5)
        return copy(number, xr.at[side, k - 1, h, part], cr.at[d, side, k - 1, part], device)

    def start_y(make):
        for d in (BELOW, ABOVE):
            @pl.when(has[1 - d])
            def _():
                make(d).start()

    def wait_y(make):
        for d in (BELOW, ABOVE):
            @pl.when(has[d])
            def _():
                make(d).wait_recv()

    for d in (BELOW, ABOVE):
        @pl.when(jnp.logical_not(has[d]))
        def _():
            myr[d] = jnp.zeros((4, 4, 128), F32)
            mcr[d] = jnp.zeros((2, 4, 4, 128), F32)

    load_fluid.wait()
    for c in range(4):
        wet = wet_in[c].astype(F32)
        marks[4 + c, pl.ds(4, 8), :] = wet
        ms[c, 0] = wet[0:4]
        ms[c, 1] = wet[4:8]

    def own(c):
        loads[c].wait()
        post = relax([f0[q, c] for q in range(19)])
        for q in range(19):
            xs[c, 0, SLOT[q]] = post[q][0:4]
            xs[c, 1, SLOT[q]] = post[q][4:8]
            grid[0, 4 + c, SLOT[q], pl.ds(4, 8), :] = post[q]

    own(3)
    pl.semaphore_wait(barrier, 1 + (gy + ny - 1) // ny + (2 * ny - 2 - gy) // ny)
    to_x(LEFT, 0).start()
    to_x(LEFT, 1).start()
    for c in (2, 1, 0):
        own(c)
        to_x(LEFT, 4 - c).start()
    start_y(lambda d: to_y(d, 0))
    start_y(lambda d: to_y(d, 1))

    def meet_left():
        to_x(LEFT, 0).wait_recv()
        for k in range(5):
            to_x(RIGHT, k).start()
        start_y(lambda d: to_corner(d, LEFT, 0))

    @pl.when(jnp.logical_not(seam))
    def _():
        meet_left()

    def unpack_marks(side):
        for c in range(4):
            col = c if side == LEFT else 8 + c
            marks[col, pl.ds(4, 4), :] = mxr[side, c, 0]
            marks[col, pl.ds(8, 4), :] = mxr[side, c, 1]
            marks[col, pl.ds(0, 4), :] = mcr[BELOW, side, c]
            marks[col, pl.ds(12, 4), :] = mcr[ABOVE, side, c]

    def unpack(side, k):
        c = 4 - k if side == LEFT else 8 + k - 1
        slots = range(19) if k < 4 else (range(14, 19) if side == LEFT else range(5))
        for s in slots:
            grid[0, c, s, pl.ds(4, 4), :] = xr[side, k - 1, 0, s]
            grid[0, c, s, pl.ds(8, 4), :] = xr[side, k - 1, 1, s]
            grid[0, c, s, pl.ds(0, 4), :] = cr[BELOW, side, k - 1, s]
            grid[0, c, s, pl.ds(12, 4), :] = cr[ABOVE, side, k - 1, s]

    wait_y(lambda d: to_y(d, 0))
    for c in range(4):
        marks[4 + c, pl.ds(0, 4), :] = myr[BELOW, c]
        marks[4 + c, pl.ds(12, 4), :] = myr[ABOVE, c]
    to_x(RIGHT, 0).wait_recv()
    start_y(lambda d: to_corner(d, RIGHT, 0))
    for k in range(1, 5):
        to_x(RIGHT, k).wait_recv()
        start_y(lambda d: to_corner(d, RIGHT, k))
    wait_y(lambda d: to_y(d, 1))

    def fill_rows(c, carry):
        for s in range(19):
            grid[0, 4 + c, s, pl.ds(0, 4), :] = yr[BELOW, c, s]
            grid[0, 4 + c, s, pl.ds(12, 4), :] = yr[ABOVE, c, s]
        return carry

    lax.fori_loop(0, 4, fill_rows, 0)
    wait_y(lambda d: to_corner(d, RIGHT, 0))
    unpack_marks(RIGHT)

    def mask_range(low, high):
        def body(col, carry):
            mask_column(marks, masks, col)
            return carry
        lax.fori_loop(low, high, body, 0)

    mask_range(5, 11)
    for k in range(1, 5):
        wait_y(lambda d: to_corner(d, RIGHT, k))
        unpack(RIGHT, k)

    for level, low, high in ((0, 5, 11), (1, 6, 10), (2, 7, 9)):
        def body(col, carry, level=level):
            column_step(grid, masks, level, col)
            return carry
        lax.fori_loop(low, high, body, 0)

    @pl.when(seam)
    def _():
        meet_left()

    for k in range(1, 5):
        to_x(LEFT, k).wait_recv()
        start_y(lambda d: to_corner(d, LEFT, k))
    wait_y(lambda d: to_corner(d, LEFT, 0))
    unpack_marks(LEFT)
    mask_range(1, 5)
    for k in range(1, 5):
        wait_y(lambda d: to_corner(d, LEFT, k))
        unpack(LEFT, k)

        def body(level, carry, k=k):
            column_step(grid, masks, level, level + 5 - k)
            return carry

        lax.fori_loop(0, 3, body, 0)
        c = 4 - k
        f = pulled(grid, masks, 3, 4 + c, 4)
        wet = wet_in[c] == 1
        for q in range(19):
            out_ref[q, c] = jnp.where(wet, f[q], f0[q, c])

    for side in (LEFT, RIGHT):
        for k in range(5):
            to_x(side, k).wait_send()
    for d in (BELOW, ABOVE):
        @pl.when(has[1 - d])
        def _():
            for k in range(2):
                to_y(d, k).wait_send()
            for side in (LEFT, RIGHT):
                for k in range(5):
                    to_corner(d, side, k).wait_send()


def per_device(nx, ny, zs, populations, fluid):
    hbm = pl.BlockSpec(memory_space=pltpu.HBM)
    vm = lambda *shape: pltpu.VMEM(shape, F32)
    return pl.pallas_call(
        functools.partial(kernel, nx, ny, zs),
        out_shape=pltpu.VMEM(populations.shape, F32),
        in_specs=[hbm, hbm],
        out_specs=pl.BlockSpec(memory_space=pltpu.VMEM),
        scratch_shapes=[
            vm(19, 4, 8, 128),
            pltpu.VMEM((4, 8, 128), jnp.int32),
            vm(4, 2, 19, 4, 128),
            vm(4, 2, 4, 128),
            vm(2, 4, 2, 19, 4, 128),
            vm(2, 4, 2, 4, 128),
            vm(2, 4, 19, 4, 128),
            vm(2, 4, 4, 128),
            vm(2, 2, 4, 19, 4, 128),
            vm(2, 2, 4, 4, 128),
            vm(4, 12, 19, 16, 128),
            vm(12, 16, 128),
            vm(12, 18, 16, 128),
            pltpu.SemaphoreType.DMA((5,)),
            pltpu.SemaphoreType.DMA((34,)),
            pltpu.SemaphoreType.DMA((34,)),
        ],
        compiler_params=pltpu.CompilerParams(
            collective_id=0, has_side_effects=True, vmem_limit_bytes=32 * 2**20
        ),
    )(*(pltpu.with_memory_space_constraint(a, pltpu.HBM) for a in (populations, fluid)))


def solution(mesh):
    nx, ny = mesh.shape["gx"], mesh.shape["gy"]
    return jax.shard_map(
        functools.partial(per_device, nx, ny, min(nx, 32)),
        mesh=mesh,
        in_specs=(P(None, "gx", "gy", None), P("gx", "gy", None)),
        out_specs=P(None, "gx", "gy", None),
        check_vma=False,
    )
```

```python
import functools

import jax
import jax.numpy as jnp
from jax import lax
from jax.experimental import pallas as pl
from jax.experimental.pallas import tpu as pltpu
from jax.sharding import PartitionSpec as P

MESH = pl.DeviceIdType.MESH
F32 = jnp.float32

VEL = [
    (0, 0, 0), (1, 0, 0), (-1, 0, 0), (0, 1, 0), (0, -1, 0), (0, 0, 1), (0, 0, -1),
    (1, 1, 0), (-1, -1, 0), (1, -1, 0), (-1, 1, 0), (1, 0, 1), (-1, 0, -1), (1, 0, -1), (-1, 0, 1),
    (0, 1, 1), (0, -1, -1), (0, 1, -1), (0, -1, 1),
]
OPP = [0, 2, 1, 4, 3, 6, 5, 8, 7, 10, 9, 12, 11, 14, 13, 16, 15, 18, 17]
OMEGA = 1.25
ORDER = [2, 8, 10, 12, 14, 0, 3, 4, 5, 6, 15, 16, 17, 18, 1, 7, 9, 11, 13]
SLOT = [ORDER.index(q) for q in range(19)]
LEFT, RIGHT = 0, 1
BELOW, ABOVE = 0, 1


def relax(f):
    even = {q: f[q] + f[q + 1] for q in range(1, 19, 2)}
    odd = {q: f[q] - f[q + 1] for q in range(1, 19, 2)}
    rho = (((f[0] + even[1]) + (even[3] + even[5])) + ((even[7] + even[9]) + (even[11] + even[13]))) + (even[15] + even[17])
    jx = (odd[1] + odd[7]) + (odd[9] + odd[11]) + odd[13]
    jy = (odd[3] + odd[7]) + (odd[15] - odd[9]) + odd[17]
    jz = (odd[5] + odd[11]) + (odd[15] - odd[13]) - odd[17]
    inv = 3.0 / rho
    v = (jx * inv, jy * inv, jz * inv)
    base = 1.0 - (v[0] * v[0] + v[1] * v[1] + v[2] * v[2]) * (1.5 / 9.0)
    out = [None] * 19
    keep = 1.0 - OMEGA
    out[0] = f[0] * keep + (rho * (OMEGA / 3.0)) * base
    for first, last, weight in ((1, 7, 1.0 / 18.0), (7, 19, 1.0 / 36.0)):
        scale = rho * (OMEGA * weight)
        level = scale * base
        half = scale * 0.5
        for q in range(first, last, 2):
            proj = None
            for axis in range(3):
                c = VEL[q][axis]
                if c:
                    term = v[axis]
                    if proj is None:
                        proj = term
                    else:
                        proj = proj + term if c > 0 else proj - term
            sym = level + half * (proj * proj)
            anti = scale * proj
            out[q] = f[q] * keep + (sym + anti)
            out[q + 1] = f[q + 1] * keep + (sym - anti)
    return out


def pulled(grid, masks, level, col, start):
    f = []
    for q in range(19):
        cx, cy, cz = VEL[q]
        src = grid[level, col - cx, SLOT[q], pl.ds(start - cy, 8), :]
        if q == 0:
            f.append(src)
            continue
        if cz:
            src = pltpu.roll(src, cz % 128, 1)
        open_ = masks[col, q - 1, pl.ds(start, 8), :] > 0.5
        f.append(jnp.where(open_, src, grid[level, col, SLOT[OPP[q]], pl.ds(start, 8), :]))
    return f


def column_steps(grid, masks, level, cols):
    for col in cols:
        for start in (1, 7):
            post = relax(pulled(grid, masks, level, col, start))
            for q in range(19):
                grid[level + 1, col, SLOT[q], pl.ds(start, 8), :] = post[q]


def mask_columns(marks, masks, cols):
    for col in cols:
        for start in (1, 7):
            for q in range(1, 19):
                cx, cy, cz = VEL[q]
                wet = marks[col - cx, pl.ds(start - cy, 8), :]
                if cz:
                    wet = pltpu.roll(wet, cz % 128, 1)
                masks[col, q - 1, pl.ds(start, 8), :] = wet


FROM_LEFT = 0
FROM_RIGHT = 4
FROM_Y = 6
LEFT_CORNER = 8
RIGHT_CORNER = 16
ARRIVALS = 20
TO_X, TO_X_SECOND, TO_ABOVE, TO_BELOW = range(4)
UNITS = {"column": 38, "far": 48, "all": 124, "rows": 80, "corner": 19, "far_corner": 24, "all_corner": 62}


def kernel(nx, ny, zs, pop_ref, fluid_ref, out_ref, f0, wet_in, xs, ms, xr, mxr, yr, myr, cr, mcr, grid, marks, masks, units,
           load_sem, send_sem, recv_sem):
    gx, gy = lax.axis_index("gx"), lax.axis_index("gy")
    right, left = lax.rem(gx + 1, nx), lax.rem(gx + nx - 1, nx)
    has = (gy > 0, gy < ny - 1)
    seam = lax.rem(gx, zs) == 0

    load_fluid = pltpu.make_async_copy(fluid_ref, wet_in, load_sem.at[0])
    load_last = pltpu.make_async_copy(pop_ref.at[:, pl.ds(3, 1)], f0.at[:, pl.ds(3, 1)], load_sem.at[1])
    load_rest = pltpu.make_async_copy(pop_ref.at[:, pl.ds(0, 3)], f0.at[:, pl.ds(0, 3)], load_sem.at[2])
    load_fluid.start()
    load_last.start()
    load_rest.start()

    barrier = pltpu.get_barrier_semaphore()
    pl.semaphore_signal(barrier, inc=1, device_id=(left, gy), device_id_type=MESH)
    for d, step in ((BELOW, -1), (ABOVE, 1)):
        @pl.when(has[d])
        def _():
            pl.semaphore_signal(barrier, inc=1, device_id=(left, gy + step), device_id_type=MESH)
            pl.semaphore_signal(barrier, inc=1, device_id=(gx, gy + step), device_id_type=MESH)

    def copy(src, dst, sent, arrived, device):
        return pltpu.make_async_remote_copy(
            src_ref=src, dst_ref=dst, send_sem=send_sem.at[sent], recv_sem=recv_sem.at[arrived],
            device_id=device, device_id_type=MESH)

    def arrive(number, count):
        part = units.at[pl.ds(0, count)]
        copy(part, part, 0, number, (right, gy)).wait_recv()

    def departed(sent, count):
        part = units.at[pl.ds(0, count)]
        copy(part, part, sent, 0, (right, gy)).wait_send()

    LEFT_PART, RIGHT_PART = pl.ds(14, 5), pl.ds(0, 5)

    def row_of(d):
        return gy + 1 if d == BELOW else gy - 1

    def start_y(make):
        for d in (BELOW, ABOVE):
            @pl.when(has[1 - d])
            def _():
                for one in make(d, 1 - d, TO_ABOVE if d == BELOW else TO_BELOW):
                    one.start()

    def wait_y(number, stride, count):
        for d in (BELOW, ABOVE):
            @pl.when(has[d])
            def _():
                arrive(number + stride * d, count)

    for d in (BELOW, ABOVE):
        @pl.when(jnp.logical_not(has[d]))
        def _():
            myr[d] = jnp.zeros((4, 4, 128), F32)
            mcr[d] = jnp.zeros((2, 4, 4, 128), F32)

    load_fluid.wait()
    for c in range(4):
        wet = wet_in[c].astype(F32)
        marks[4 + c, pl.ds(4, 8), :] = wet
        ms[c, 0] = wet[0:4]
        ms[c, 1] = wet[4:8]

    def own(c):
        post = relax([f0[q, c] for q in range(19)])
        for q in range(19):
            xs[c, 0, SLOT[q]] = post[q][0:4]
            xs[c, 1, SLOT[q]] = post[q][4:8]
            grid[0, 4 + c, SLOT[q], pl.ds(4, 8), :] = post[q]

    load_last.wait()
    own(3)
    pl.semaphore_wait(barrier, 1 + 2 * ((gy + ny - 1) // ny) + 2 * ((2 * ny - 2 - gy) // ny))
    to_right = (right, gy)
    copy(ms, mxr.at[LEFT], TO_X, FROM_LEFT, to_right).start()
    copy(xs.at[3], xr.at[LEFT, 0], TO_X, FROM_LEFT + 1, to_right).start()
    load_rest.wait()
    own(2)
    second = copy(xs.at[2], xr.at[LEFT, 1], TO_X_SECOND, FROM_LEFT + 2, to_right)
    second.start()
    own(1)
    copy(xs.at[1], xr.at[LEFT, 2], TO_X, FROM_LEFT + 3, to_right).start()
    own(0)
    copy(xs.at[0, :, LEFT_PART], xr.at[LEFT, 3, :, LEFT_PART], TO_X, FROM_LEFT + 3, to_right).start()
    start_y(lambda d, h, sent: [copy(ms.at[:, h], myr.at[d], sent, FROM_Y + d, (gx, row_of(d)))])
    second.wait_send()
    start_y(lambda d, h, sent: [
        copy(xs.at[1, h], cr.at[d, LEFT, 2], sent, LEFT_CORNER + 4 * d + 3, (right, row_of(d))),
        copy(xs.at[0, h, LEFT_PART], cr.at[d, LEFT, 3, LEFT_PART], sent, LEFT_CORNER + 4 * d + 3, (right, row_of(d))),
        copy(xs.at[:, h], yr.at[d], sent, FROM_Y + d, (gx, row_of(d))),
    ])

    def meet_left():
        arrive(FROM_LEFT, 8)
        to_left = (left, gy)
        copy(ms, mxr.at[RIGHT], TO_X, FROM_RIGHT, to_left).start()
        copy(xs.at[pl.ds(0, 3)], xr.at[RIGHT, pl.ds(0, 3)], TO_X, FROM_RIGHT + 1, to_left).start()
        copy(xs.at[3, :, RIGHT_PART], xr.at[RIGHT, 3, :, RIGHT_PART], TO_X, FROM_RIGHT + 1, to_left).start()
        start_y(lambda d, h, sent: [
            copy(mxr.at[LEFT, :, h], mcr.at[d, LEFT], sent, LEFT_CORNER + 4 * d, (gx, row_of(d)))])

    @pl.when(jnp.logical_not(seam))
    def _():
        meet_left()

    def unpack_marks(side):
        for c in range(4):
            col = c if side == LEFT else 8 + c
            marks[col, pl.ds(4, 4), :] = mxr[side, c, 0]
            marks[col, pl.ds(8, 4), :] = mxr[side, c, 1]
            marks[col, pl.ds(0, 4), :] = mcr[BELOW, side, c]
            marks[col, pl.ds(12, 4), :] = mcr[ABOVE, side, c]

    def unpack(side, k):
        c = 4 - k if side == LEFT else 8 + k - 1
        slots = range(19) if k < 4 else (range(14, 19) if side == LEFT else range(5))
        for s in slots:
            grid[0, c, s, pl.ds(4, 4), :] = xr[side, k - 1, 0, s]
            grid[0, c, s, pl.ds(8, 4), :] = xr[side, k - 1, 1, s]
            grid[0, c, s, pl.ds(0, 4), :] = cr[BELOW, side, k - 1, s]
            grid[0, c, s, pl.ds(12, 4), :] = cr[ABOVE, side, k - 1, s]

    def loop(count, make):
        def body(i, carry):
            make(i)
            return carry
        lax.fori_loop(0, count, body, 0)

    arrive(FROM_RIGHT, 8)
    start_y(lambda d, h, sent: [
        copy(mxr.at[RIGHT, :, h], mcr.at[d, RIGHT], sent, RIGHT_CORNER + 2 * d, (gx, row_of(d)))])
    arrive(FROM_RIGHT + 1, UNITS["all"])
    start_y(lambda d, h, sent: [
        copy(xr.at[RIGHT, pl.ds(0, 3), h], cr.at[d, RIGHT, pl.ds(0, 3)], sent, RIGHT_CORNER + 2 * d + 1, (gx, row_of(d))),
        copy(xr.at[RIGHT, 3, h, RIGHT_PART], cr.at[d, RIGHT, 3, RIGHT_PART], sent, RIGHT_CORNER + 2 * d + 1, (gx, row_of(d))),
    ])
    wait_y(FROM_Y, 1, UNITS["rows"])
    for c in range(4):
        marks[4 + c, pl.ds(0, 4), :] = myr[BELOW, c]
        marks[4 + c, pl.ds(12, 4), :] = myr[ABOVE, c]

    def fill_rows(c):
        for s in range(19):
            grid[0, 4 + c, s, pl.ds(0, 4), :] = yr[BELOW, c, s]
            grid[0, 4 + c, s, pl.ds(12, 4), :] = yr[ABOVE, c, s]

    loop(4, fill_rows)
    wait_y(RIGHT_CORNER, 2, 4)
    unpack_marks(RIGHT)
    loop(3, lambda i: mask_columns(marks, masks, (5 + 2 * i, 6 + 2 * i)))
    wait_y(RIGHT_CORNER + 1, 2, UNITS["all_corner"])
    for k in range(1, 5):
        unpack(RIGHT, k)

    loop(3, lambda i: column_steps(grid, masks, 0, (5 + 2 * i, 6 + 2 * i)))

    @pl.when(seam)
    def _():
        meet_left()

    def pass_on(k):
        arrive(FROM_LEFT + k, UNITS["column"])
        start_y(lambda d, h, sent: [
            copy(xr.at[LEFT, k - 1, h], cr.at[d, LEFT, k - 1], sent, LEFT_CORNER + 4 * d + k, (gx, row_of(d)))])

    pass_on(1)
    loop(2, lambda i: column_steps(grid, masks, 1, (6 + 2 * i, 7 + 2 * i)))
    pass_on(2)
    column_steps(grid, masks, 2, (7, 8))

    wait_y(LEFT_CORNER, 4, 4)
    unpack_marks(LEFT)
    loop(2, lambda i: mask_columns(marks, masks, (1 + 2 * i, 2 + 2 * i)))

    def finish(c):
        f = pulled(grid, masks, 3, 4 + c, 4)
        wet = wet_in[c] == 1
        for q in range(19):
            out_ref[q, c] = jnp.where(wet, f[q], f0[q, c])

    for k in (1, 2):
        wait_y(LEFT_CORNER + k, 4, UNITS["corner"])
        unpack(LEFT, k)
        loop(3, lambda level: column_steps(grid, masks, level, (level + 5 - k,)))
        finish(4 - k)
    arrive(FROM_LEFT + 3, UNITS["far"])
    wait_y(LEFT_CORNER + 3, 4, UNITS["far_corner"])
    unpack(LEFT, 3)
    unpack(LEFT, 4)
    loop(3, lambda level: column_steps(grid, masks, level, (level + 1, level + 2)))
    finish(1)
    finish(0)

    departed(TO_X, 8 + 38 + UNITS["far"] + 8 + UNITS["all"])
    for d in (BELOW, ABOVE):
        @pl.when(has[1 - d])
        def _():
            departed(
                TO_ABOVE if d == BELOW else TO_BELOW,
                UNITS["rows"] + 4 + 2 * UNITS["corner"] + UNITS["far_corner"] + 4 + UNITS["all_corner"])


def per_device(nx, ny, zs, populations, fluid):
    hbm = pl.BlockSpec(memory_space=pltpu.HBM)
    vm = lambda *shape: pltpu.VMEM(shape, F32)
    return pl.pallas_call(
        functools.partial(kernel, nx, ny, zs),
        out_shape=pltpu.VMEM(populations.shape, F32),
        in_specs=[hbm, hbm],
        out_specs=pl.BlockSpec(memory_space=pltpu.VMEM),
        scratch_shapes=[
            vm(19, 4, 8, 128),
            pltpu.VMEM((4, 8, 128), jnp.int32),
            vm(4, 2, 19, 4, 128),
            vm(4, 2, 4, 128),
            vm(2, 4, 2, 19, 4, 128),
            vm(2, 4, 2, 4, 128),
            vm(2, 4, 19, 4, 128),
            vm(2, 4, 4, 128),
            vm(2, 2, 4, 19, 4, 128),
            vm(2, 2, 4, 4, 128),
            vm(4, 12, 19, 16, 128),
            vm(12, 16, 128),
            vm(12, 18, 16, 128),
            vm(256, 4, 128),
            pltpu.SemaphoreType.DMA((3,)),
            pltpu.SemaphoreType.DMA((4,)),
            pltpu.SemaphoreType.DMA((ARRIVALS,)),
        ],
        compiler_params=pltpu.CompilerParams(
            collective_id=0, has_side_effects=True, vmem_limit_bytes=32 * 2**20
        ),
    )(*(pltpu.with_memory_space_constraint(a, pltpu.HBM) for a in (populations, fluid)))


def solution(mesh):
    nx, ny = mesh.shape["gx"], mesh.shape["gy"]
    return jax.shard_map(
        functools.partial(per_device, nx, ny, min(nx, 32)),
        mesh=mesh,
        in_specs=(P(None, "gx", "gy", None), P("gx", "gy", None)),
        out_specs=P(None, "gx", "gy", None),
        check_vma=False,
    )
```

```python
import functools

import jax
import jax.numpy as jnp
from jax import lax
from jax.experimental import pallas as pl
from jax.experimental.pallas import tpu as pltpu
from jax.sharding import PartitionSpec as P

MESH = pl.DeviceIdType.MESH
F32 = jnp.float32

VEL = [
    (0, 0, 0), (1, 0, 0), (-1, 0, 0), (0, 1, 0), (0, -1, 0), (0, 0, 1), (0, 0, -1),
    (1, 1, 0), (-1, -1, 0), (1, -1, 0), (-1, 1, 0), (1, 0, 1), (-1, 0, -1), (1, 0, -1), (-1, 0, 1),
    (0, 1, 1), (0, -1, -1), (0, 1, -1), (0, -1, 1),
]
OPP = [0, 2, 1, 4, 3, 6, 5, 8, 7, 10, 9, 12, 11, 14, 13, 16, 15, 18, 17]
OMEGA = 1.25
ORDER = [2, 8, 10, 12, 14, 0, 3, 4, 5, 6, 15, 16, 17, 18, 1, 7, 9, 11, 13]
SLOT = [ORDER.index(q) for q in range(19)]
LEFT, RIGHT = 0, 1
BELOW, ABOVE = 0, 1


def relax(f, wanted=range(19)):
    even = {q: f[q] + f[q + 1] for q in range(1, 19, 2)}
    odd = {q: f[q] - f[q + 1] for q in range(1, 19, 2)}
    rho = (((f[0] + even[1]) + (even[3] + even[5])) + ((even[7] + even[9]) + (even[11] + even[13]))) + (even[15] + even[17])
    jx = (odd[1] + odd[7]) + (odd[9] + odd[11]) + odd[13]
    jy = (odd[3] + odd[7]) + (odd[15] - odd[9]) + odd[17]
    jz = (odd[5] + odd[11]) + (odd[15] - odd[13]) - odd[17]
    inv = 3.0 / rho
    v = (jx * inv, jy * inv, jz * inv)
    base = 1.0 - (v[0] * v[0] + v[1] * v[1] + v[2] * v[2]) * (1.5 / 9.0)
    out = [None] * 19
    keep = 1.0 - OMEGA
    if 0 in wanted:
        out[0] = f[0] * keep + (rho * (OMEGA / 3.0)) * base
    for first, last, weight in ((1, 7, 1.0 / 18.0), (7, 19, 1.0 / 36.0)):
        scale = rho * (OMEGA * weight)
        level = scale * base
        half = scale * 0.5
        for q in range(first, last, 2):
            proj = None
            for axis in range(3):
                c = VEL[q][axis]
                if c:
                    term = v[axis]
                    if proj is None:
                        proj = term
                    else:
                        proj = proj + term if c > 0 else proj - term
            sym = level + half * (proj * proj)
            anti = scale * proj
            if q in wanted:
                out[q] = f[q] * keep + (sym + anti)
            if q + 1 in wanted:
                out[q + 1] = f[q + 1] * keep + (sym - anti)
    return out


def pulled(grid, masks, level, col, start):
    f = []
    for q in range(19):
        cx, cy, cz = VEL[q]
        src = grid[level, col - cx, SLOT[q], pl.ds(start - cy, 8), :]
        if q == 0:
            f.append(src)
            continue
        if cz:
            src = pltpu.roll(src, cz % 128, 1)
        open_ = masks[col, q - 1, pl.ds(start, 8), :] > 0.5
        f.append(jnp.where(open_, src, grid[level, col, SLOT[OPP[q]], pl.ds(start, 8), :]))
    return f


def column_steps(grid, masks, level, cols, wanted=range(19)):
    for col in cols:
        for start in (1, 7):
            post = relax(pulled(grid, masks, level, col, start), wanted)
            for q in wanted:
                grid[level + 1, col, SLOT[q], pl.ds(start, 8), :] = post[q]


def mask_columns(marks, masks, cols):
    for col in cols:
        for start in (1, 7):
            for q in range(1, 19):
                cx, cy, cz = VEL[q]
                wet = marks[col - cx, pl.ds(start - cy, 8), :]
                if cz:
                    wet = pltpu.roll(wet, cz % 128, 1)
                masks[col, q - 1, pl.ds(start, 8), :] = wet


FROM_LEFT = 0
FROM_RIGHT = 6
FROM_Y = 8
LEFT_CORNER = 10
RIGHT_CORNER = 18
ARRIVALS = 22
TO_X, TO_X_SECOND, TO_ABOVE, TO_BELOW = range(4)
UNITS = {"column": 38, "far": 48, "all": 124, "rows": 80, "corner": 19, "far_corner": 24, "all_corner": 62}


def kernel(nx, ny, zs, pop_ref, fluid_ref, out_ref, f0, wet_in, xs, ms, xr, mxr, yr, myr, cr, mcr, grid, marks, masks, units,
           load_sem, send_sem, recv_sem):
    gx, gy = lax.axis_index("gx"), lax.axis_index("gy")
    right, left = lax.rem(gx + 1, nx), lax.rem(gx + nx - 1, nx)
    has = (gy > 0, gy < ny - 1)
    seam = lax.rem(gx, zs) == 0

    barrier = pltpu.get_barrier_semaphore()
    for d, step in ((BELOW, -1), (ABOVE, 1)):
        @pl.when(has[d])
        def _():
            pl.semaphore_signal(barrier, inc=1, device_id=(gx, gy + step), device_id_type=MESH)
            pl.semaphore_signal(barrier, inc=1, device_id=(left, gy + step), device_id_type=MESH)
    pl.semaphore_signal(barrier, inc=1, device_id=(left, gy), device_id_type=MESH)

    load_fluid = pltpu.make_async_copy(fluid_ref, wet_in, load_sem.at[0])
    load_last = pltpu.make_async_copy(pop_ref.at[:, pl.ds(3, 1)], f0.at[:, pl.ds(3, 1)], load_sem.at[1])
    load_rest = pltpu.make_async_copy(pop_ref.at[:, pl.ds(0, 3)], f0.at[:, pl.ds(0, 3)], load_sem.at[2])
    load_fluid.start()
    load_last.start()
    load_rest.start()

    def copy(src, dst, sent, arrived, device):
        return pltpu.make_async_remote_copy(
            src_ref=src, dst_ref=dst, send_sem=send_sem.at[sent], recv_sem=recv_sem.at[arrived],
            device_id=device, device_id_type=MESH)

    def arrive(number, count):
        part = units.at[pl.ds(0, count)]
        copy(part, part, 0, number, (right, gy)).wait_recv()

    def departed(sent, count):
        part = units.at[pl.ds(0, count)]
        copy(part, part, sent, 0, (right, gy)).wait_send()

    LEFT_PART, RIGHT_PART = pl.ds(14, 5), pl.ds(0, 5)

    def row_of(d):
        return gy + 1 if d == BELOW else gy - 1

    def start_y(make):
        for d in (BELOW, ABOVE):
            @pl.when(has[1 - d])
            def _():
                for one in make(d, 1 - d, TO_ABOVE if d == BELOW else TO_BELOW):
                    one.start()

    def wait_y(number, stride, count):
        for d in (BELOW, ABOVE):
            @pl.when(has[d])
            def _():
                arrive(number + stride * d, count)

    for d in (BELOW, ABOVE):
        @pl.when(jnp.logical_not(has[d]))
        def _():
            myr[d] = jnp.zeros((4, 4, 128), F32)
            mcr[d] = jnp.zeros((2, 4, 4, 128), F32)

    load_fluid.wait()
    for c in range(4):
        wet = wet_in[c].astype(F32)
        marks[4 + c, pl.ds(4, 8), :] = wet
        ms[c, 0] = wet[0:4]
        ms[c, 1] = wet[4:8]

    def own(c):
        post = relax([f0[q, c] for q in range(19)])
        for q in range(19):
            xs[c, 0, SLOT[q]] = post[q][0:4]
            xs[c, 1, SLOT[q]] = post[q][4:8]
            grid[0, 4 + c, SLOT[q], pl.ds(4, 8), :] = post[q]

    load_last.wait()
    own(3)
    pl.semaphore_wait(barrier, 1 + 2 * ((gy + ny - 1) // ny) + 2 * ((2 * ny - 2 - gy) // ny))
    to_right = (right, gy)
    copy(xs.at[3, 0], xr.at[LEFT, 0, 0], TO_X, FROM_LEFT + 1, to_right).start()
    copy(ms, mxr.at[LEFT], TO_X, FROM_LEFT, to_right).start()
    copy(xs.at[3, 1], xr.at[LEFT, 0, 1], TO_X, FROM_LEFT + 2, to_right).start()
    load_rest.wait()
    own(2)
    second = copy(xs.at[2, 0], xr.at[LEFT, 1, 0], TO_X_SECOND, FROM_LEFT + 3, to_right)
    second.start()
    copy(xs.at[2, 1], xr.at[LEFT, 1, 1], TO_X, FROM_LEFT + 4, to_right).start()
    own(1)
    copy(xs.at[1], xr.at[LEFT, 2], TO_X, FROM_LEFT + 5, to_right).start()
    own(0)
    copy(xs.at[0, :, LEFT_PART], xr.at[LEFT, 3, :, LEFT_PART], TO_X, FROM_LEFT + 5, to_right).start()
    start_y(lambda d, h, sent: [copy(ms.at[:, h], myr.at[d], sent, FROM_Y + d, (gx, row_of(d)))])
    second.wait_send()
    start_y(lambda d, h, sent: [
        copy(xs.at[1, h], cr.at[d, LEFT, 2], sent, LEFT_CORNER + 4 * d + 3, (right, row_of(d))),
        copy(xs.at[0, h, LEFT_PART], cr.at[d, LEFT, 3, LEFT_PART], sent, LEFT_CORNER + 4 * d + 3, (right, row_of(d))),
        copy(xs.at[:, h], yr.at[d], sent, FROM_Y + d, (gx, row_of(d))),
    ])

    def meet_left():
        arrive(FROM_LEFT, 8)
        to_left = (left, gy)
        copy(ms, mxr.at[RIGHT], TO_X, FROM_RIGHT, to_left).start()
        copy(xs.at[pl.ds(0, 3)], xr.at[RIGHT, pl.ds(0, 3)], TO_X, FROM_RIGHT + 1, to_left).start()
        copy(xs.at[3, :, RIGHT_PART], xr.at[RIGHT, 3, :, RIGHT_PART], TO_X, FROM_RIGHT + 1, to_left).start()
        start_y(lambda d, h, sent: [
            copy(mxr.at[LEFT, :, h], mcr.at[d, LEFT], sent, LEFT_CORNER + 4 * d, (gx, row_of(d)))])

    @pl.when(jnp.logical_not(seam))
    def _():
        meet_left()

    def unpack_marks(side):
        for c in range(4):
            col = c if side == LEFT else 8 + c
            marks[col, pl.ds(4, 4), :] = mxr[side, c, 0]
            marks[col, pl.ds(8, 4), :] = mxr[side, c, 1]
            marks[col, pl.ds(0, 4), :] = mcr[BELOW, side, c]
            marks[col, pl.ds(12, 4), :] = mcr[ABOVE, side, c]

    def unpack(side, k):
        c = 4 - k if side == LEFT else 8 + k - 1
        slots = range(19) if k < 4 else (range(14, 19) if side == LEFT else range(5))
        for s in slots:
            grid[0, c, s, pl.ds(4, 4), :] = xr[side, k - 1, 0, s]
            grid[0, c, s, pl.ds(8, 4), :] = xr[side, k - 1, 1, s]
            grid[0, c, s, pl.ds(0, 4), :] = cr[BELOW, side, k - 1, s]
            grid[0, c, s, pl.ds(12, 4), :] = cr[ABOVE, side, k - 1, s]

    def loop(count, make):
        def body(i, carry):
            make(i)
            return carry
        lax.fori_loop(0, count, body, 0)

    arrive(FROM_RIGHT, 8)
    start_y(lambda d, h, sent: [
        copy(mxr.at[RIGHT, :, h], mcr.at[d, RIGHT], sent, RIGHT_CORNER + 2 * d, (gx, row_of(d)))])
    arrive(FROM_RIGHT + 1, UNITS["all"])
    start_y(lambda d, h, sent: [
        copy(xr.at[RIGHT, pl.ds(0, 3), h], cr.at[d, RIGHT, pl.ds(0, 3)], sent, RIGHT_CORNER + 2 * d + 1, (gx, row_of(d))),
        copy(xr.at[RIGHT, 3, h, RIGHT_PART], cr.at[d, RIGHT, 3, RIGHT_PART], sent, RIGHT_CORNER + 2 * d + 1, (gx, row_of(d))),
    ])
    wait_y(FROM_Y, 1, UNITS["rows"])
    for c in range(4):
        marks[4 + c, pl.ds(0, 4), :] = myr[BELOW, c]
        marks[4 + c, pl.ds(12, 4), :] = myr[ABOVE, c]

    def fill_rows(c):
        for s in range(19):
            grid[0, 4 + c, s, pl.ds(0, 4), :] = yr[BELOW, c, s]
            grid[0, 4 + c, s, pl.ds(12, 4), :] = yr[ABOVE, c, s]

    loop(4, fill_rows)
    wait_y(RIGHT_CORNER, 2, 4)
    unpack_marks(RIGHT)
    loop(3, lambda i: mask_columns(marks, masks, (5 + 2 * i, 6 + 2 * i)))
    wait_y(RIGHT_CORNER + 1, 2, UNITS["all_corner"])
    for k in range(1, 5):
        unpack(RIGHT, k)

    def pass_on(k, h):
        arrive(FROM_LEFT + 2 * k - 1 + h, UNITS["corner"])
        d = 1 - h

        @pl.when(has[h])
        def _():
            copy(xr.at[LEFT, k - 1, h], cr.at[d, LEFT, k - 1], TO_ABOVE if d == BELOW else TO_BELOW, LEFT_CORNER + 4 * d + k,
                 (gx, row_of(d))).start()

    pass_on(1, 0)

    @pl.when(seam)
    def _():
        meet_left()

    loop(3, lambda i: column_steps(grid, masks, 0, (5 + 2 * i, 6 + 2 * i)))
    pass_on(1, 1)
    loop(2, lambda i: column_steps(grid, masks, 1, (6 + 2 * i, 7 + 2 * i)))
    pass_on(2, 0)
    column_steps(grid, masks, 2, (7, 8))
    pass_on(2, 1)

    wait_y(LEFT_CORNER, 4, 4)
    unpack_marks(LEFT)
    loop(2, lambda i: mask_columns(marks, masks, (1 + 2 * i, 2 + 2 * i)))

    def finish(c):
        f = pulled(grid, masks, 3, 4 + c, 4)
        wet = wet_in[c] == 1
        for q in range(19):
            out_ref[q, c] = jnp.where(wet, f[q], f0[q, c])

    wait_y(LEFT_CORNER + 1, 4, UNITS["corner"])
    unpack(LEFT, 1)
    loop(3, lambda level: column_steps(grid, masks, level, (level + 4,)))
    finish(3)
    arrive(FROM_LEFT + 5, UNITS["far"])
    wait_y(LEFT_CORNER + 2, 4, UNITS["corner"])
    wait_y(LEFT_CORNER + 3, 4, UNITS["far_corner"])
    for k in (2, 3, 4):
        unpack(LEFT, k)

    def last_wave(level):
        column_steps(grid, masks, level, (level + 1,), ORDER[14:])
        column_steps(grid, masks, level, (level + 2, level + 3))

    loop(3, last_wave)
    for c in (2, 1, 0):
        finish(c)

    departed(TO_X, 8 + 38 + 19 + UNITS["far"] + 8 + UNITS["all"])
    for d in (BELOW, ABOVE):
        @pl.when(has[1 - d])
        def _():
            departed(
                TO_ABOVE if d == BELOW else TO_BELOW,
                UNITS["rows"] + 4 + 2 * UNITS["corner"] + UNITS["far_corner"] + 4 + UNITS["all_corner"])


def per_device(nx, ny, zs, populations, fluid):
    hbm = pl.BlockSpec(memory_space=pltpu.HBM)
    vm = lambda *shape: pltpu.VMEM(shape, F32)
    return pl.pallas_call(
        functools.partial(kernel, nx, ny, zs),
        out_shape=pltpu.VMEM(populations.shape, F32),
        in_specs=[hbm, hbm],
        out_specs=pl.BlockSpec(memory_space=pltpu.VMEM),
        scratch_shapes=[
            vm(19, 4, 8, 128),
            pltpu.VMEM((4, 8, 128), jnp.int32),
            vm(4, 2, 19, 4, 128),
            vm(4, 2, 4, 128),
            vm(2, 4, 2, 19, 4, 128),
            vm(2, 4, 2, 4, 128),
            vm(2, 4, 19, 4, 128),
            vm(2, 4, 4, 128),
            vm(2, 2, 4, 19, 4, 128),
            vm(2, 2, 4, 4, 128),
            vm(4, 12, 19, 16, 128),
            vm(12, 16, 128),
            vm(12, 18, 16, 128),
            vm(256, 4, 128),
            pltpu.SemaphoreType.DMA((3,)),
            pltpu.SemaphoreType.DMA((4,)),
            pltpu.SemaphoreType.DMA((ARRIVALS,)),
        ],
        compiler_params=pltpu.CompilerParams(
            collective_id=0, has_side_effects=True, vmem_limit_bytes=32 * 2**20
        ),
    )(*(pltpu.with_memory_space_constraint(a, pltpu.HBM) for a in (populations, fluid)))


def solution(mesh):
    nx, ny = mesh.shape["gx"], mesh.shape["gy"]
    return jax.shard_map(
        functools.partial(per_device, nx, ny, min(nx, 32)),
        mesh=mesh,
        in_specs=(P(None, "gx", "gy", None), P("gx", "gy", None)),
        out_specs=P(None, "gx", "gy", None),
        check_vma=False,
    )
```

```python
import functools

import jax
import jax.numpy as jnp
from jax import lax
from jax.experimental import pallas as pl
from jax.experimental.pallas import tpu as pltpu
from jax.sharding import PartitionSpec as P

MESH = pl.DeviceIdType.MESH
F32 = jnp.float32

VEL = [
    (0, 0, 0), (1, 0, 0), (-1, 0, 0), (0, 1, 0), (0, -1, 0), (0, 0, 1), (0, 0, -1),
    (1, 1, 0), (-1, -1, 0), (1, -1, 0), (-1, 1, 0), (1, 0, 1), (-1, 0, -1), (1, 0, -1), (-1, 0, 1),
    (0, 1, 1), (0, -1, -1), (0, 1, -1), (0, -1, 1),
]
OPP = [0, 2, 1, 4, 3, 6, 5, 8, 7, 10, 9, 12, 11, 14, 13, 16, 15, 18, 17]
OMEGA = 1.25
ORDER = [2, 8, 10, 12, 14, 0, 3, 4, 5, 6, 15, 16, 17, 18, 1, 7, 9, 11, 13]
SLOT = [ORDER.index(q) for q in range(19)]
LEFT, RIGHT = 0, 1
BELOW, ABOVE = 0, 1


def relax(f, wanted=range(19)):
    even = {q: f[q] + f[q + 1] for q in range(1, 19, 2)}
    odd = {q: f[q] - f[q + 1] for q in range(1, 19, 2)}
    rho = (((f[0] + even[1]) + (even[3] + even[5])) + ((even[7] + even[9]) + (even[11] + even[13]))) + (even[15] + even[17])
    jx = (odd[1] + odd[7]) + (odd[9] + odd[11]) + odd[13]
    jy = (odd[3] + odd[7]) + (odd[15] - odd[9]) + odd[17]
    jz = (odd[5] + odd[11]) + (odd[15] - odd[13]) - odd[17]
    inv = 3.0 / rho
    v = (jx * inv, jy * inv, jz * inv)
    base = 1.0 - (v[0] * v[0] + v[1] * v[1] + v[2] * v[2]) * (1.5 / 9.0)
    out = [None] * 19
    keep = 1.0 - OMEGA
    if 0 in wanted:
        out[0] = f[0] * keep + (rho * (OMEGA / 3.0)) * base
    for first, last, weight in ((1, 7, 1.0 / 18.0), (7, 19, 1.0 / 36.0)):
        scale = rho * (OMEGA * weight)
        level = scale * base
        half = scale * 0.5
        for q in range(first, last, 2):
            proj = None
            for axis in range(3):
                c = VEL[q][axis]
                if c:
                    term = v[axis]
                    if proj is None:
                        proj = term
                    else:
                        proj = proj + term if c > 0 else proj - term
            sym = level + half * (proj * proj)
            anti = scale * proj
            if q in wanted:
                out[q] = f[q] * keep + (sym + anti)
            if q + 1 in wanted:
                out[q + 1] = f[q + 1] * keep + (sym - anti)
    return out


def pulled(grid, masks, level, col, start):
    f = []
    for q in range(19):
        cx, cy, cz = VEL[q]
        src = grid[level, col - cx, SLOT[q], pl.ds(start - cy, 8), :]
        if q == 0:
            f.append(src)
            continue
        if cz:
            src = pltpu.roll(src, cz % 128, 1)
        open_ = masks[col, q - 1, pl.ds(start, 8), :] > 0.5
        f.append(jnp.where(open_, src, grid[level, col, SLOT[OPP[q]], pl.ds(start, 8), :]))
    return f


def column_steps(grid, masks, level, cols, wanted=range(19)):
    for col in cols:
        for start in (1, 7):
            post = relax(pulled(grid, masks, level, col, start), wanted)
            for q in wanted:
                grid[level + 1, col, SLOT[q], pl.ds(start, 8), :] = post[q]


def mask_columns(marks, masks, cols):
    for col in cols:
        for start in (1, 7):
            for q in range(1, 19):
                cx, cy, cz = VEL[q]
                wet = marks[col - cx, pl.ds(start - cy, 8), :]
                if cz:
                    wet = pltpu.roll(wet, cz % 128, 1)
                masks[col, q - 1, pl.ds(start, 8), :] = wet


FROM_LEFT = 0
FROM_RIGHT = 6
FROM_Y = 8
LEFT_CORNER = 10
RIGHT_CORNER = 18
RELAY = 22
ARRIVALS = 26
TO_X, TO_X_SECOND, TO_ABOVE, TO_BELOW, NEAR_ABOVE, NEAR_BELOW, RELAYED = range(7)
UNITS = {"column": 38, "far": 48, "all": 124, "rows": 80, "corner": 19, "far_corner": 24, "all_corner": 62}


def kernel(nx, ny, zs, pop_ref, fluid_ref, out_ref, f0, wet_in, xs, ms, xr, mxr, yr, myr, cr, mcr, grid, marks, masks, units, relay,
           load_sem, send_sem, recv_sem):
    gx, gy = lax.axis_index("gx"), lax.axis_index("gy")
    right, left = lax.rem(gx + 1, nx), lax.rem(gx + nx - 1, nx)
    has = (gy > 0, gy < ny - 1)
    place = lax.rem(gx, zs)
    seam, helper, late = place == 0, place == 1, place == zs - 1
    right2, left2 = lax.rem(gx + 2, nx), lax.rem(gx + nx - 2, nx)

    barrier = pltpu.get_barrier_semaphore()
    for d, step in ((BELOW, -1), (ABOVE, 1)):
        @pl.when(has[d])
        def _():
            pl.semaphore_signal(barrier, inc=1, device_id=(gx, gy + step), device_id_type=MESH)
            pl.semaphore_signal(barrier, inc=1, device_id=(left, gy + step), device_id_type=MESH)
    pl.semaphore_signal(barrier, inc=1, device_id=(left, gy), device_id_type=MESH)

    @pl.when(helper)
    def _():
        pl.semaphore_signal(barrier, inc=1, device_id=(left2, gy), device_id_type=MESH)

    load_fluid = pltpu.make_async_copy(fluid_ref, wet_in, load_sem.at[0])
    load_last = pltpu.make_async_copy(pop_ref.at[:, pl.ds(3, 1)], f0.at[:, pl.ds(3, 1)], load_sem.at[1])
    load_rest = pltpu.make_async_copy(pop_ref.at[:, pl.ds(0, 3)], f0.at[:, pl.ds(0, 3)], load_sem.at[2])
    load_fluid.start()
    load_last.start()
    load_rest.start()

    def copy(src, dst, sent, arrived, device):
        return pltpu.make_async_remote_copy(
            src_ref=src, dst_ref=dst, send_sem=send_sem.at[sent], recv_sem=recv_sem.at[arrived],
            device_id=device, device_id_type=MESH)

    def arrive(number, count):
        part = units.at[pl.ds(0, count)]
        copy(part, part, 0, number, (right, gy)).wait_recv()

    def departed(sent, count):
        part = units.at[pl.ds(0, count)]
        copy(part, part, sent, 0, (right, gy)).wait_send()

    LEFT_PART, RIGHT_PART = pl.ds(14, 5), pl.ds(0, 5)

    def row_of(d):
        return gy + 1 if d == BELOW else gy - 1

    def start_y(make):
        for d in (BELOW, ABOVE):
            @pl.when(has[1 - d])
            def _():
                for one in make(d, 1 - d, TO_ABOVE if d == BELOW else TO_BELOW):
                    one.start()

    def wait_y(number, stride, count):
        for d in (BELOW, ABOVE):
            @pl.when(has[d])
            def _():
                arrive(number + stride * d, count)

    for d in (BELOW, ABOVE):
        @pl.when(jnp.logical_not(has[d]))
        def _():
            myr[d] = jnp.zeros((4, 4, 128), F32)
            mcr[d] = jnp.zeros((2, 4, 4, 128), F32)

    load_fluid.wait()
    for c in range(4):
        wet = wet_in[c].astype(F32)
        marks[4 + c, pl.ds(4, 8), :] = wet
        ms[c, 0] = wet[0:4]
        ms[c, 1] = wet[4:8]

    def own(c):
        post = relax([f0[q, c] for q in range(19)])
        for q in range(19):
            xs[c, 0, SLOT[q]] = post[q][0:4]
            xs[c, 1, SLOT[q]] = post[q][4:8]
            grid[0, 4 + c, SLOT[q], pl.ds(4, 8), :] = post[q]

    load_last.wait()
    own(3)
    beside = (gy + ny - 1) // ny + (2 * ny - 2 - gy) // ny
    pl.semaphore_wait(barrier, 1 + 2 * beside + place // (zs - 1))
    to_right = (right, gy)

    def near(k, h, sent):
        @pl.when(late)
        def _():
            copy(xs.at[4 - k, h], relay.at[k - 1, h], sent, RELAY + 2 * k - 2 + h, (right2, gy)).start()

        @pl.when(jnp.logical_not(late))
        def _():
            copy(xs.at[4 - k, h], xr.at[LEFT, k - 1, h], sent, FROM_LEFT + 2 * k - 1 + h, to_right).start()

    near(1, 0, TO_X_SECOND)
    copy(ms, mxr.at[LEFT], TO_X, FROM_LEFT, to_right).start()
    near(1, 1, TO_X)
    load_rest.wait()
    own(2)
    near(2, 0, TO_X)
    near(2, 1, TO_X)
    own(1)
    copy(xs.at[1], xr.at[LEFT, 2], TO_X, FROM_LEFT + 5, to_right).start()
    own(0)
    copy(xs.at[0, :, LEFT_PART], xr.at[LEFT, 3, :, LEFT_PART], TO_X, FROM_LEFT + 5, to_right).start()
    start_y(lambda d, h, sent: [copy(ms.at[:, h], myr.at[d], sent, FROM_Y + d, (gx, row_of(d)))])
    departed(TO_X_SECOND, UNITS["corner"])
    start_y(lambda d, h, sent: [
        copy(xs.at[1, h], cr.at[d, LEFT, 2], sent, LEFT_CORNER + 4 * d + 3, (right, row_of(d))),
        copy(xs.at[0, h, LEFT_PART], cr.at[d, LEFT, 3, LEFT_PART], sent, LEFT_CORNER + 4 * d + 3, (right, row_of(d))),
    ])

    def send_rows():
        start_y(lambda d, h, sent: [copy(xs.at[:, h], yr.at[d], sent, FROM_Y + d, (gx, row_of(d)))])

    @pl.when(place < zs - 2)
    def _():
        send_rows()

    def meet_left():
        arrive(FROM_LEFT, 8)
        to_left = (left, gy)
        copy(ms, mxr.at[RIGHT], TO_X, FROM_RIGHT, to_left).start()
        copy(xs.at[pl.ds(0, 3)], xr.at[RIGHT, pl.ds(0, 3)], TO_X, FROM_RIGHT + 1, to_left).start()
        copy(xs.at[3, :, RIGHT_PART], xr.at[RIGHT, 3, :, RIGHT_PART], TO_X, FROM_RIGHT + 1, to_left).start()
        start_y(lambda d, h, sent: [
            copy(mxr.at[LEFT, :, h], mcr.at[d, LEFT], sent, LEFT_CORNER + 4 * d, (gx, row_of(d)))])

    @pl.when(jnp.logical_not(seam))
    def _():
        meet_left()

    @pl.when(place >= zs - 2)
    def _():
        send_rows()

    def unpack_marks(side):
        for c in range(4):
            col = c if side == LEFT else 8 + c
            marks[col, pl.ds(4, 4), :] = mxr[side, c, 0]
            marks[col, pl.ds(8, 4), :] = mxr[side, c, 1]
            marks[col, pl.ds(0, 4), :] = mcr[BELOW, side, c]
            marks[col, pl.ds(12, 4), :] = mcr[ABOVE, side, c]

    def unpack(side, k):
        c = 4 - k if side == LEFT else 8 + k - 1
        slots = range(19) if k < 4 else (range(14, 19) if side == LEFT else range(5))
        for s in slots:
            grid[0, c, s, pl.ds(4, 4), :] = xr[side, k - 1, 0, s]
            grid[0, c, s, pl.ds(8, 4), :] = xr[side, k - 1, 1, s]
            grid[0, c, s, pl.ds(0, 4), :] = cr[BELOW, side, k - 1, s]
            grid[0, c, s, pl.ds(12, 4), :] = cr[ABOVE, side, k - 1, s]

    def loop(count, make):
        def body(i, carry):
            make(i)
            return carry
        lax.fori_loop(0, count, body, 0)

    arrive(FROM_RIGHT, 8)
    start_y(lambda d, h, sent: [
        copy(mxr.at[RIGHT, :, h], mcr.at[d, RIGHT], sent, RIGHT_CORNER + 2 * d, (gx, row_of(d)))])
    arrive(FROM_RIGHT + 1, UNITS["all"])
    start_y(lambda d, h, sent: [
        copy(xr.at[RIGHT, pl.ds(0, 3), h], cr.at[d, RIGHT, pl.ds(0, 3)], sent, RIGHT_CORNER + 2 * d + 1, (gx, row_of(d))),
        copy(xr.at[RIGHT, 3, h, RIGHT_PART], cr.at[d, RIGHT, 3, RIGHT_PART], sent, RIGHT_CORNER + 2 * d + 1, (gx, row_of(d))),
    ])
    wait_y(FROM_Y, 1, UNITS["rows"])
    for c in range(4):
        marks[4 + c, pl.ds(0, 4), :] = myr[BELOW, c]
        marks[4 + c, pl.ds(12, 4), :] = myr[ABOVE, c]

    def fill_rows(c):
        for s in range(19):
            grid[0, 4 + c, s, pl.ds(0, 4), :] = yr[BELOW, c, s]
            grid[0, 4 + c, s, pl.ds(12, 4), :] = yr[ABOVE, c, s]

    loop(4, fill_rows)
    wait_y(RIGHT_CORNER, 2, 4)
    unpack_marks(RIGHT)
    loop(3, lambda i: mask_columns(marks, masks, (5 + 2 * i, 6 + 2 * i)))
    wait_y(RIGHT_CORNER + 1, 2, UNITS["all_corner"])
    for k in range(1, 5):
        unpack(RIGHT, k)

    def pass_on(k, h):
        d = 1 - h

        @pl.when(jnp.logical_not(seam))
        def _():
            arrive(FROM_LEFT + 2 * k - 1 + h, UNITS["corner"])

        @pl.when(jnp.logical_and(jnp.logical_not(seam), has[h]))
        def _():
            copy(xr.at[LEFT, k - 1, h], cr.at[d, LEFT, k - 1], NEAR_ABOVE if d == BELOW else NEAR_BELOW, LEFT_CORNER + 4 * d + k,
                 (gx, row_of(d))).start()

    pass_on(1, 0)

    @pl.when(seam)
    def _():
        meet_left()

    loop(3, lambda i: column_steps(grid, masks, 0, (5 + 2 * i, 6 + 2 * i)))
    pass_on(1, 1)
    loop(2, lambda i: column_steps(grid, masks, 1, (6 + 2 * i, 7 + 2 * i)))
    pass_on(2, 0)
    column_steps(grid, masks, 2, (7, 8))
    pass_on(2, 1)

    @pl.when(helper)
    def _():
        for k in (1, 2):
            for h in (0, 1):
                arrive(RELAY + 2 * k - 2 + h, UNITS["corner"])
                d = 1 - h

                @pl.when(has[h])
                def _():
                    copy(relay.at[k - 1, h], cr.at[d, LEFT, k - 1], RELAYED, LEFT_CORNER + 4 * d + k, (left, row_of(d))).start()

                copy(relay.at[k - 1, h], xr.at[LEFT, k - 1, h], RELAYED, FROM_LEFT + 2 * k - 1 + h, (left, gy)).start()

    def near_arrived(k):
        @pl.when(seam)
        def _():
            for h in (0, 1):
                arrive(FROM_LEFT + 2 * k - 1 + h, UNITS["corner"])

    wait_y(LEFT_CORNER, 4, 4)
    unpack_marks(LEFT)
    loop(2, lambda i: mask_columns(marks, masks, (1 + 2 * i, 2 + 2 * i)))

    def finish(c):
        f = pulled(grid, masks, 3, 4 + c, 4)
        wet = wet_in[c] == 1
        for q in range(19):
            out_ref[q, c] = jnp.where(wet, f[q], f0[q, c])

    near_arrived(1)
    wait_y(LEFT_CORNER + 1, 4, UNITS["corner"])
    unpack(LEFT, 1)
    loop(3, lambda level: column_steps(grid, masks, level, (level + 4,)))
    finish(3)
    near_arrived(2)
    wait_y(LEFT_CORNER + 2, 4, UNITS["corner"])
    unpack(LEFT, 2)
    arrive(FROM_LEFT + 5, UNITS["far"])
    wait_y(LEFT_CORNER + 3, 4, UNITS["far_corner"])
    unpack(LEFT, 3)
    unpack(LEFT, 4)

    def last_wave(level):
        column_steps(grid, masks, level, (level + 1,), ORDER[14:])
        column_steps(grid, masks, level, (level + 2, level + 3))

    loop(3, last_wave)
    for c in (2, 1, 0):
        finish(c)

    departed(TO_X, 8 + 38 + 19 + UNITS["far"] + 8 + UNITS["all"])
    for d in (BELOW, ABOVE):
        @pl.when(has[1 - d])
        def _():
            departed(
                TO_ABOVE if d == BELOW else TO_BELOW,
                UNITS["rows"] + 4 + UNITS["far_corner"] + 4 + UNITS["all_corner"])

        @pl.when(jnp.logical_and(jnp.logical_not(seam), has[1 - d]))
        def _():
            departed(NEAR_ABOVE if d == BELOW else NEAR_BELOW, 2 * UNITS["corner"])

    both = jnp.logical_and(has[BELOW], has[ABOVE])

    @pl.when(jnp.logical_and(helper, both))
    def _():
        departed(RELAYED, 8 * UNITS["corner"])

    @pl.when(jnp.logical_and(helper, jnp.logical_not(both)))
    def _():
        departed(RELAYED, 6 * UNITS["corner"])


def per_device(nx, ny, zs, populations, fluid):
    hbm = pl.BlockSpec(memory_space=pltpu.HBM)
    vm = lambda *shape: pltpu.VMEM(shape, F32)
    return pl.pallas_call(
        functools.partial(kernel, nx, ny, zs),
        out_shape=pltpu.VMEM(populations.shape, F32),
        in_specs=[hbm, hbm],
        out_specs=pl.BlockSpec(memory_space=pltpu.VMEM),
        scratch_shapes=[
            vm(19, 4, 8, 128),
            pltpu.VMEM((4, 8, 128), jnp.int32),
            vm(4, 2, 19, 4, 128),
            vm(4, 2, 4, 128),
            vm(2, 4, 2, 19, 4, 128),
            vm(2, 4, 2, 4, 128),
            vm(2, 4, 19, 4, 128),
            vm(2, 4, 4, 128),
            vm(2, 2, 4, 19, 4, 128),
            vm(2, 2, 4, 4, 128),
            vm(4, 12, 19, 16, 128),
            vm(12, 16, 128),
            vm(12, 18, 16, 128),
            vm(256, 4, 128),
            vm(2, 2, 19, 4, 128),
            pltpu.SemaphoreType.DMA((3,)),
            pltpu.SemaphoreType.DMA((7,)),
            pltpu.SemaphoreType.DMA((ARRIVALS,)),
        ],
        compiler_params=pltpu.CompilerParams(
            collective_id=0, has_side_effects=True, vmem_limit_bytes=32 * 2**20
        ),
    )(*(pltpu.with_memory_space_constraint(a, pltpu.HBM) for a in (populations, fluid)))


def solution(mesh):
    nx, ny = mesh.shape["gx"], mesh.shape["gy"]
    return jax.shard_map(
        functools.partial(per_device, nx, ny, min(nx, 32)),
        mesh=mesh,
        in_specs=(P(None, "gx", "gy", None), P("gx", "gy", None)),
        out_specs=P(None, "gx", "gy", None),
        check_vma=False,
    )
```

```python
import functools

import jax
import jax.numpy as jnp
from jax import lax
from jax.experimental import pallas as pl
from jax.experimental.pallas import tpu as pltpu
from jax.sharding import PartitionSpec as P

MESH = pl.DeviceIdType.MESH
F32 = jnp.float32

VEL = [
    (0, 0, 0), (1, 0, 0), (-1, 0, 0), (0, 1, 0), (0, -1, 0), (0, 0, 1), (0, 0, -1),
    (1, 1, 0), (-1, -1, 0), (1, -1, 0), (-1, 1, 0), (1, 0, 1), (-1, 0, -1), (1, 0, -1), (-1, 0, 1),
    (0, 1, 1), (0, -1, -1), (0, 1, -1), (0, -1, 1),
]
OPP = [0, 2, 1, 4, 3, 6, 5, 8, 7, 10, 9, 12, 11, 14, 13, 16, 15, 18, 17]
OMEGA = 1.25
ORDER = [2, 8, 10, 12, 14, 0, 3, 4, 5, 6, 15, 16, 17, 18, 1, 7, 9, 11, 13]
SLOT = [ORDER.index(q) for q in range(19)]
LEFT, RIGHT = 0, 1
BELOW, ABOVE = 0, 1


def relax(f, wanted=range(19)):
    even = {q: f[q] + f[q + 1] for q in range(1, 19, 2)}
    odd = {q: f[q] - f[q + 1] for q in range(1, 19, 2)}
    rho = (((f[0] + even[1]) + (even[3] + even[5])) + ((even[7] + even[9]) + (even[11] + even[13]))) + (even[15] + even[17])
    jx = (odd[1] + odd[7]) + (odd[9] + odd[11]) + odd[13]
    jy = (odd[3] + odd[7]) + (odd[15] - odd[9]) + odd[17]
    jz = (odd[5] + odd[11]) + (odd[15] - odd[13]) - odd[17]
    inv = 3.0 / rho
    v = (jx * inv, jy * inv, jz * inv)
    base = 1.0 - (v[0] * v[0] + v[1] * v[1] + v[2] * v[2]) * (1.5 / 9.0)
    out = [None] * 19
    keep = 1.0 - OMEGA
    if 0 in wanted:
        out[0] = f[0] * keep + (rho * (OMEGA / 3.0)) * base
    for first, last, weight in ((1, 7, 1.0 / 18.0), (7, 19, 1.0 / 36.0)):
        scale = rho * (OMEGA * weight)
        level = scale * base
        half = scale * 0.5
        for q in range(first, last, 2):
            proj = None
            for axis in range(3):
                c = VEL[q][axis]
                if c:
                    term = v[axis]
                    if proj is None:
                        proj = term
                    else:
                        proj = proj + term if c > 0 else proj - term
            sym = level + half * (proj * proj)
            anti = scale * proj
            if q in wanted:
                out[q] = f[q] * keep + (sym + anti)
            if q + 1 in wanted:
                out[q + 1] = f[q + 1] * keep + (sym - anti)
    return out


def pulled(grid, masks, level, col, start):
    f = []
    for q in range(19):
        cx, cy, cz = VEL[q]
        src = grid[level, col - cx, SLOT[q], pl.ds(start - cy, 8), :]
        if q == 0:
            f.append(src)
            continue
        if cz:
            src = pltpu.roll(src, cz % 128, 1)
        open_ = masks[col, q - 1, pl.ds(start, 8), :] > 0.5
        f.append(jnp.where(open_, src, grid[level, col, SLOT[OPP[q]], pl.ds(start, 8), :]))
    return f


def column_steps(grid, masks, level, cols, wanted=range(19)):
    for col in cols:
        for start in (1, 7):
            post = relax(pulled(grid, masks, level, col, start), wanted)
            for q in wanted:
                grid[level + 1, col, SLOT[q], pl.ds(start, 8), :] = post[q]


def mask_columns(marks, masks, cols):
    for col in cols:
        for start in (1, 7):
            for q in range(1, 19):
                cx, cy, cz = VEL[q]
                wet = marks[col - cx, pl.ds(start - cy, 8), :]
                if cz:
                    wet = pltpu.roll(wet, cz % 128, 1)
                masks[col, q - 1, pl.ds(start, 8), :] = wet


FROM_LEFT = 0
FROM_RIGHT = 6
FROM_Y = 8
LEFT_CORNER = 10
RIGHT_CORNER = 18
RELAY = 22
ARRIVALS = 26
TO_X, TO_X_SECOND, TO_ABOVE, TO_BELOW, NEAR_ABOVE, NEAR_BELOW, RELAYED = range(7)
UNITS = {"column": 38, "far": 48, "all": 124, "rows": 80, "corner": 19, "far_corner": 24, "all_corner": 62}


def kernel(nx, ny, zs, pop_ref, fluid_ref, out_ref, f0, wet_in, xs, ms, xr, mxr, yr, myr, cr, mcr, grid, marks, masks, units, relay,
           load_sem, send_sem, recv_sem):
    gx, gy = lax.axis_index("gx"), lax.axis_index("gy")
    right, left = lax.rem(gx + 1, nx), lax.rem(gx + nx - 1, nx)
    has = (gy > 0, gy < ny - 1)
    place = lax.rem(gx, zs)
    seam, helper, late = place == 0, place == 1, place == zs - 1
    right2, left2 = lax.rem(gx + 2, nx), lax.rem(gx + nx - 2, nx)

    barrier = pltpu.get_barrier_semaphore()
    for d, step in ((BELOW, -1), (ABOVE, 1)):
        @pl.when(has[d])
        def _():
            pl.semaphore_signal(barrier, inc=1, device_id=(gx, gy + step), device_id_type=MESH)
            pl.semaphore_signal(barrier, inc=1, device_id=(left, gy + step), device_id_type=MESH)
    pl.semaphore_signal(barrier, inc=1, device_id=(left, gy), device_id_type=MESH)

    @pl.when(helper)
    def _():
        pl.semaphore_signal(barrier, inc=1, device_id=(left2, gy), device_id_type=MESH)

    load_fluid = pltpu.make_async_copy(fluid_ref, wet_in, load_sem.at[0])
    load_last = pltpu.make_async_copy(pop_ref.at[:, pl.ds(3, 1)], f0.at[:, pl.ds(3, 1)], load_sem.at[1])
    load_rest = pltpu.make_async_copy(pop_ref.at[:, pl.ds(0, 3)], f0.at[:, pl.ds(0, 3)], load_sem.at[2])
    load_fluid.start()
    load_last.start()
    load_rest.start()

    def copy(src, dst, sent, arrived, device):
        return pltpu.make_async_remote_copy(
            src_ref=src, dst_ref=dst, send_sem=send_sem.at[sent], recv_sem=recv_sem.at[arrived],
            device_id=device, device_id_type=MESH)

    def arrive(number, count):
        part = units.at[pl.ds(0, count)]
        copy(part, part, 0, number, (right, gy)).wait_recv()

    def departed(sent, count):
        part = units.at[pl.ds(0, count)]
        copy(part, part, sent, 0, (right, gy)).wait_send()

    LEFT_PART, RIGHT_PART = pl.ds(14, 5), pl.ds(0, 5)

    def row_of(d):
        return gy + 1 if d == BELOW else gy - 1

    def start_y(make):
        for d in (BELOW, ABOVE):
            @pl.when(has[1 - d])
            def _():
                for one in make(d, 1 - d, TO_ABOVE if d == BELOW else TO_BELOW):
                    one.start()

    def wait_y(number, stride, count):
        for d in (BELOW, ABOVE):
            @pl.when(has[d])
            def _():
                arrive(number + stride * d, count)

    for d in (BELOW, ABOVE):
        @pl.when(jnp.logical_not(has[d]))
        def _():
            myr[d] = jnp.zeros((4, 4, 128), F32)
            mcr[d] = jnp.zeros((2, 4, 4, 128), F32)

    load_fluid.wait()
    for c in range(4):
        wet = wet_in[c].astype(F32)
        marks[4 + c, pl.ds(4, 8), :] = wet
        ms[c, 0] = wet[0:4]
        ms[c, 1] = wet[4:8]

    def own(c):
        post = relax([f0[q, c] for q in range(19)])
        for q in range(19):
            xs[c, 0, SLOT[q]] = post[q][0:4]
            xs[c, 1, SLOT[q]] = post[q][4:8]
            grid[0, 4 + c, SLOT[q], pl.ds(4, 8), :] = post[q]

    load_last.wait()
    own(3)
    beside = (gy + ny - 1) // ny + (2 * ny - 2 - gy) // ny
    pl.semaphore_wait(barrier, 1 + 2 * beside + place // (zs - 1))
    to_right = (right, gy)

    def near(k, h, sent):
        @pl.when(late)
        def _():
            copy(xs.at[4 - k, h], relay.at[k - 1, h], sent, RELAY + 2 * k - 2 + h, (right2, gy)).start()

        @pl.when(jnp.logical_not(late))
        def _():
            copy(xs.at[4 - k, h], xr.at[LEFT, k - 1, h], sent, FROM_LEFT + 2 * k - 1 + h, to_right).start()

    near(1, 0, TO_X_SECOND)
    copy(ms, mxr.at[LEFT], TO_X, FROM_LEFT, to_right).start()
    near(1, 1, TO_X)
    load_rest.wait()
    own(2)
    near(2, 0, TO_X)
    near(2, 1, TO_X)
    own(1)
    copy(xs.at[1], xr.at[LEFT, 2], TO_X, FROM_LEFT + 5, to_right).start()
    own(0)
    copy(xs.at[0, :, LEFT_PART], xr.at[LEFT, 3, :, LEFT_PART], TO_X, FROM_LEFT + 5, to_right).start()
    start_y(lambda d, h, sent: [copy(ms.at[:, h], myr.at[d], sent, FROM_Y + d, (gx, row_of(d)))])
    departed(TO_X_SECOND, UNITS["corner"])
    start_y(lambda d, h, sent: [
        copy(xs.at[1, h], cr.at[d, LEFT, 2], sent, LEFT_CORNER + 4 * d + 3, (right, row_of(d))),
        copy(xs.at[0, h, LEFT_PART], cr.at[d, LEFT, 3, LEFT_PART], sent, LEFT_CORNER + 4 * d + 3, (right, row_of(d))),
    ])

    def send_rows():
        start_y(lambda d, h, sent: [copy(xs.at[:, h], yr.at[d], sent, FROM_Y + d, (gx, row_of(d)))])

    @pl.when(place < zs - 2)
    def _():
        send_rows()

    def meet_left():
        arrive(FROM_LEFT, 8)
        to_left = (left, gy)
        copy(ms, mxr.at[RIGHT], TO_X, FROM_RIGHT, to_left).start()
        copy(xs.at[pl.ds(0, 3)], xr.at[RIGHT, pl.ds(0, 3)], TO_X, FROM_RIGHT + 1, to_left).start()
        copy(xs.at[3, :, RIGHT_PART], xr.at[RIGHT, 3, :, RIGHT_PART], TO_X, FROM_RIGHT + 1, to_left).start()
        start_y(lambda d, h, sent: [
            copy(mxr.at[LEFT, :, h], mcr.at[d, LEFT], sent, LEFT_CORNER + 4 * d, (gx, row_of(d)))])

    @pl.when(jnp.logical_not(seam))
    def _():
        meet_left()

    @pl.when(place >= zs - 2)
    def _():
        send_rows()

    def unpack_marks(side):
        for c in range(4):
            col = c if side == LEFT else 8 + c
            marks[col, pl.ds(4, 4), :] = mxr[side, c, 0]
            marks[col, pl.ds(8, 4), :] = mxr[side, c, 1]
            marks[col, pl.ds(0, 4), :] = mcr[BELOW, side, c]
            marks[col, pl.ds(12, 4), :] = mcr[ABOVE, side, c]

    def place_of(side, k):
        slots = range(19) if k < 4 else (range(14, 19) if side == LEFT else range(5))
        return 4 - k if side == LEFT else 8 + k - 1, slots

    def unpack_own_rows(side, k):
        c, slots = place_of(side, k)
        for s in slots:
            grid[0, c, s, pl.ds(4, 4), :] = xr[side, k - 1, 0, s]
            grid[0, c, s, pl.ds(8, 4), :] = xr[side, k - 1, 1, s]

    def unpack_corners(side, k):
        c, slots = place_of(side, k)
        for s in slots:
            grid[0, c, s, pl.ds(0, 4), :] = cr[BELOW, side, k - 1, s]
            grid[0, c, s, pl.ds(12, 4), :] = cr[ABOVE, side, k - 1, s]

    def loop(count, make):
        def body(i, carry):
            make(i)
            return carry
        lax.fori_loop(0, count, body, 0)

    arrive(FROM_RIGHT, 8)
    start_y(lambda d, h, sent: [
        copy(mxr.at[RIGHT, :, h], mcr.at[d, RIGHT], sent, RIGHT_CORNER + 2 * d, (gx, row_of(d)))])
    arrive(FROM_RIGHT + 1, UNITS["all"])
    start_y(lambda d, h, sent: [
        copy(xr.at[RIGHT, pl.ds(0, 3), h], cr.at[d, RIGHT, pl.ds(0, 3)], sent, RIGHT_CORNER + 2 * d + 1, (gx, row_of(d))),
        copy(xr.at[RIGHT, 3, h, RIGHT_PART], cr.at[d, RIGHT, 3, RIGHT_PART], sent, RIGHT_CORNER + 2 * d + 1, (gx, row_of(d))),
    ])
    wait_y(FROM_Y, 1, UNITS["rows"])
    for c in range(4):
        marks[4 + c, pl.ds(0, 4), :] = myr[BELOW, c]
        marks[4 + c, pl.ds(12, 4), :] = myr[ABOVE, c]

    def fill_rows(c):
        for s in range(19):
            grid[0, 4 + c, s, pl.ds(0, 4), :] = yr[BELOW, c, s]
            grid[0, 4 + c, s, pl.ds(12, 4), :] = yr[ABOVE, c, s]

    loop(4, fill_rows)
    wait_y(RIGHT_CORNER, 2, 4)
    unpack_marks(RIGHT)
    loop(3, lambda i: mask_columns(marks, masks, (5 + 2 * i, 6 + 2 * i)))
    wait_y(RIGHT_CORNER + 1, 2, UNITS["all_corner"])
    for k in range(1, 5):
        unpack_own_rows(RIGHT, k)
        unpack_corners(RIGHT, k)

    def pass_on(k, h):
        d = 1 - h

        @pl.when(jnp.logical_not(seam))
        def _():
            arrive(FROM_LEFT + 2 * k - 1 + h, UNITS["corner"])

        @pl.when(jnp.logical_and(jnp.logical_not(seam), has[h]))
        def _():
            copy(xr.at[LEFT, k - 1, h], cr.at[d, LEFT, k - 1], NEAR_ABOVE if d == BELOW else NEAR_BELOW, LEFT_CORNER + 4 * d + k,
                 (gx, row_of(d))).start()

    pass_on(1, 0)

    @pl.when(seam)
    def _():
        meet_left()

    loop(3, lambda i: column_steps(grid, masks, 0, (5 + 2 * i, 6 + 2 * i)))
    pass_on(1, 1)
    loop(2, lambda i: column_steps(grid, masks, 1, (6 + 2 * i, 7 + 2 * i)))
    pass_on(2, 0)
    column_steps(grid, masks, 2, (7, 8))
    pass_on(2, 1)

    @pl.when(helper)
    def _():
        for k in (1, 2):
            for h in (0, 1):
                arrive(RELAY + 2 * k - 2 + h, UNITS["corner"])
                d = 1 - h

                @pl.when(has[h])
                def _():
                    copy(relay.at[k - 1, h], cr.at[d, LEFT, k - 1], RELAYED, LEFT_CORNER + 4 * d + k, (left, row_of(d))).start()

                copy(relay.at[k - 1, h], xr.at[LEFT, k - 1, h], RELAYED, FROM_LEFT + 2 * k - 1 + h, (left, gy)).start()

    def near_arrived(k):
        @pl.when(seam)
        def _():
            for h in (0, 1):
                arrive(FROM_LEFT + 2 * k - 1 + h, UNITS["corner"])

    wait_y(LEFT_CORNER, 4, 4)
    unpack_marks(LEFT)
    loop(2, lambda i: mask_columns(marks, masks, (1 + 2 * i, 2 + 2 * i)))

    def finish(c):
        f = pulled(grid, masks, 3, 4 + c, 4)
        wet = wet_in[c] == 1
        for q in range(19):
            out_ref[q, c] = jnp.where(wet, f[q], f0[q, c])

    near_arrived(1)
    near_arrived(2)
    arrive(FROM_LEFT + 5, UNITS["far"])
    for k in range(1, 5):
        unpack_own_rows(LEFT, k)
    wait_y(LEFT_CORNER + 1, 4, UNITS["corner"])
    unpack_corners(LEFT, 1)
    loop(3, lambda level: column_steps(grid, masks, level, (level + 4,)))
    finish(3)
    wait_y(LEFT_CORNER + 2, 4, UNITS["corner"])
    unpack_corners(LEFT, 2)
    wait_y(LEFT_CORNER + 3, 4, UNITS["far_corner"])
    unpack_corners(LEFT, 3)
    unpack_corners(LEFT, 4)

    def last_wave(level):
        column_steps(grid, masks, level, (level + 1,), ORDER[14:])
        column_steps(grid, masks, level, (level + 2, level + 3))

    loop(3, last_wave)
    for c in (2, 1, 0):
        finish(c)

    departed(TO_X, 8 + 38 + 19 + UNITS["far"] + 8 + UNITS["all"])
    for d in (BELOW, ABOVE):
        @pl.when(has[1 - d])
        def _():
            departed(
                TO_ABOVE if d == BELOW else TO_BELOW,
                UNITS["rows"] + 4 + UNITS["far_corner"] + 4 + UNITS["all_corner"])

        @pl.when(jnp.logical_and(jnp.logical_not(seam), has[1 - d]))
        def _():
            departed(NEAR_ABOVE if d == BELOW else NEAR_BELOW, 2 * UNITS["corner"])

    both = jnp.logical_and(has[BELOW], has[ABOVE])

    @pl.when(jnp.logical_and(helper, both))
    def _():
        departed(RELAYED, 8 * UNITS["corner"])

    @pl.when(jnp.logical_and(helper, jnp.logical_not(both)))
    def _():
        departed(RELAYED, 6 * UNITS["corner"])


def per_device(nx, ny, zs, populations, fluid):
    hbm = pl.BlockSpec(memory_space=pltpu.HBM)
    vm = lambda *shape: pltpu.VMEM(shape, F32)
    return pl.pallas_call(
        functools.partial(kernel, nx, ny, zs),
        out_shape=pltpu.VMEM(populations.shape, F32),
        in_specs=[hbm, hbm],
        out_specs=pl.BlockSpec(memory_space=pltpu.VMEM),
        scratch_shapes=[
            vm(19, 4, 8, 128),
            pltpu.VMEM((4, 8, 128), jnp.int32),
            vm(4, 2, 19, 4, 128),
            vm(4, 2, 4, 128),
            vm(2, 4, 2, 19, 4, 128),
            vm(2, 4, 2, 4, 128),
            vm(2, 4, 19, 4, 128),
            vm(2, 4, 4, 128),
            vm(2, 2, 4, 19, 4, 128),
            vm(2, 2, 4, 4, 128),
            vm(4, 12, 19, 16, 128),
            vm(12, 16, 128),
            vm(12, 18, 16, 128),
            vm(256, 4, 128),
            vm(2, 2, 19, 4, 128),
            pltpu.SemaphoreType.DMA((3,)),
            pltpu.SemaphoreType.DMA((7,)),
            pltpu.SemaphoreType.DMA((ARRIVALS,)),
        ],
        compiler_params=pltpu.CompilerParams(
            collective_id=0, has_side_effects=True, vmem_limit_bytes=32 * 2**20
        ),
    )(*(pltpu.with_memory_space_constraint(a, pltpu.HBM) for a in (populations, fluid)))


def solution(mesh):
    nx, ny = mesh.shape["gx"], mesh.shape["gy"]
    return jax.shard_map(
        functools.partial(per_device, nx, ny, min(nx, 32)),
        mesh=mesh,
        in_specs=(P(None, "gx", "gy", None), P("gx", "gy", None)),
        out_specs=P(None, "gx", "gy", None),
        check_vma=False,
    )
```
